32 devices in a mesh: seq: 8 (over z, y), head: 4 (over x, core).
Axes of the slice: x: 2, y: 2, z: 4, core: 2. Of those that a mesh axis runs over, the one named last changes fastest.
Arguments:
- layer_in: bfloat16 [4096, 2048], P('seq'), may hold values from -6 to 6
- gain_one: float32 [2048], replicated, may hold values from 0.5 to 1.5
- w_query: bfloat16 [2048, 2048], P(None, 'head'), may hold values from -0.125 to 0.125
- w_key: bfloat16 [2048, 2048], P(None, 'head'), may hold values from -0.125 to 0.125
- w_value: bfloat16 [2048, 4096], P(None, 'head'), may hold values from -0.125 to 0.125
- w_gate: bfloat16 [2048, 4096], P(None, 'head'), may hold values from -0.125 to 0.125
- w_out: bfloat16 [4096, 2048], P('head'), may hold values from -0.15625 to 0.15625
- gain_two: float32 [2048], replicated, may hold values from 0.5 to 1.5
- w_ffgate: bfloat16 [2048, 3456], P(None, 'head'), may hold values from -0.125 to 0.125
- w_ffup: bfloat16 [2048, 3456], P(None, 'head'), may hold values from -0.125 to 0.125
- w_down: bfloat16 [3456, 2048], P('head'), may hold values from -0.1875 to 0.1875
- cotangent: bfloat16 [4096, 2048], P('seq'), may hold values from -6 to 6
Outputs:
- layer_out: bfloat16 [4096, 2048], P('seq')
- grad_input: float32 [4096, 2048], P('seq')
- grad_gain_one: float32 [2048], P('seq')
- grad_query: float32 [2048, 2048], P('seq', 'head')
- grad_key: float32 [2048, 2048], P('seq', 'head')
- grad_value: float32 [2048, 4096], P('seq', 'head')
- grad_gate: float32 [2048, 4096], P('seq', 'head')
- grad_out: float32 [4096, 2048], P('head', 'seq')
- grad_gain_two: float32 [2048], P('seq')
- grad_ffgate: float32 [2048, 3456], P('seq', 'head')
- grad_ffup: float32 [2048, 3456], P('seq', 'head')
- grad_down: float32 [3456, 2048], P('head', 'seq')
The draws below stay inside these ranges and needn't reach their ends.
All inputs are finite; a program needn't handle non-finite values.
Results may differ from the reference program's by a relative error of at most 0.015.
Values sent between devices are 32-bit elements; how exact they have to be, the bound alone decides.
A program may use at most 256 MiB of HBM per device.

```python
import jax
import jax.numpy as jnp
from jax import lax

D = 2048
HEADS = 8
DK = 256
DV = 512
FF = 3456
TOK_DEV = 512
LENGTH = 2048
TOKENS = 4096


def raised(values, key, source, target, shards_of, factor):
    def block_of(position):
        return (jnp.arange(values.shape[position]) // (values.shape[position] // shards_of)).reshape((-1,) + (1,) * (values.ndim - 1 - position))

    near = jax.random.permutation(key, shards_of)[block_of(target)]
    second = (block_of(target) + shards_of // 2) % shards_of
    return jnp.where((block_of(source) == near) | (block_of(source) == second), factor * values, values)


def shard_levels(own_key, extent, pieces, smallest, top_value):
    def one(position, parts):
        heights = jax.random.uniform(jax.random.fold_in(jax.random.fold_in(own_key, 6), position), (parts,), jnp.float32, smallest / len(pieces), top_value / len(pieces))
        return jnp.repeat(jnp.exp(heights), extent[position] // parts).reshape((-1,) + (1,) * (len(extent) - position - 1))

    factor_of = one(*pieces[0])
    for cut in pieces[1:]:
        factor_of = factor_of * one(*cut)
    return factor_of


def scatter_about(own_key, shape, spread, reach, split=(), held_as=jnp.bfloat16):
    gain = shard_levels(own_key, shape, split, -0.22, 0.18) if split else 1.0
    array = jax.random.normal(own_key, shape, jnp.float32) * spread * gain
    return jnp.minimum(jnp.maximum(array, -reach), reach).astype(held_as)


def bell_draw_with(stream_key, shape, spread, most, cuts, heavy, kind=jnp.bfloat16):
    entries = spread * jax.random.normal(stream_key, shape, jnp.float32)
    if cuts:
        entries = entries * shard_levels(stream_key, shape, cuts, -0.22, 0.18)
    return jnp.clip(raised(entries, jax.random.fold_in(stream_key, 3), *heavy), -most, most).astype(kind)


def setup_inputs(seed: int = 0) -> dict:
    keys = jax.random.split(jax.random.key(seed), 13)
    layer_in = bell_draw_with(keys[0], (TOKENS, D), 1.0, 6.0, ((0, 8),), (0, 1, 8, 2.0))
    gain_one = jnp.clip(1.0 + 0.1 * jax.random.normal(keys[1], (D,), jnp.float32), 0.5, 1.5)
    w_query = scatter_about(keys[2], (D, HEADS * DK), D ** -0.5, 0.125, ((1, 4),))
    w_key = scatter_about(keys[3], (D, HEADS * DK), D ** -0.5, 0.125, ((1, 4),))
    w_value = scatter_about(keys[4], (D, HEADS * DV), D ** -0.5, 0.125, ((1, 4),))
    w_gate = scatter_about(keys[5], (D, HEADS * DV), D ** -0.5, 0.125, ((1, 4),))
    w_out = scatter_about(keys[6], (HEADS * DV, D), (HEADS * DV // 3) ** -0.5, 0.15625, ((0, 4),))
    gain_two = jnp.clip(1.0 + 0.1 * jax.random.normal(keys[7], (D,), jnp.float32), 0.5, 1.5)
    w_ffgate = scatter_about(keys[8], (D, FF), D ** -0.5, 0.125, ((1, 4),))
    w_ffup = scatter_about(keys[9], (D, FF), D ** -0.5, 0.125, ((1, 4),))
    w_down = scatter_about(keys[10], (FF, D), (FF // 3) ** -0.5, 0.1875, ((0, 4),))
    cotangent = bell_draw_with(keys[11], (TOKENS, D), 1.0, 6.0, ((0, 8),), (0, 1, 8, 2.0))
    return {"layer_in": layer_in, "gain_one": gain_one, "w_query": w_query, "w_key": w_key, "w_value": w_value, "w_gate": w_gate, "w_out": w_out, "gain_two": gain_two, "w_ffgate": w_ffgate, "w_ffup": w_ffup, "w_down": w_down, "cotangent": cotangent}


EPS = 1e-05
ROPE_BASE = 10000.0
PRECISE = lax.Precision.HIGHEST

def rotation(positions, half_dim):
    frequency = ROPE_BASE ** (-jnp.arange(half_dim, dtype=jnp.float32) / half_dim)
    angles = positions.astype(jnp.float32)[:, None] * frequency[None, :]
    return (jnp.cos(angles), jnp.sin(angles))

def rotate(values, cos_part, sin_part):
    half_dim = cos_part.shape[1]
    leading = values[..., :half_dim]
    trailing = values[..., half_dim:]
    cos_wide = cos_part[:, None, :]
    sin_wide = sin_part[:, None, :]
    return jnp.concatenate([leading * cos_wide - trailing * sin_wide, trailing * cos_wide + leading * sin_wide], axis=-1)

def unrotate(gradient, cos_part, sin_part):
    half_dim = cos_part.shape[1]
    leading = gradient[..., :half_dim]
    trailing = gradient[..., half_dim:]
    cos_wide = cos_part[:, None, :]
    sin_wide = sin_part[:, None, :]
    return jnp.concatenate([leading * cos_wide + trailing * sin_wide, trailing * cos_wide - leading * sin_wide], axis=-1)

def rms_forward(inputs, gain_vec):
    recip = lax.rsqrt(lax.optimization_barrier(jnp.mean(inputs * inputs, axis=-1, keepdims=True)) + EPS)
    return (recip, (inputs * recip * gain_vec).astype(jnp.bfloat16))

def rms_backward(inputs, recip, gain_vec, upstream):
    weighted = upstream * gain_vec
    inner_mean = lax.optimization_barrier(jnp.mean(weighted * inputs, axis=-1, keepdims=True))
    grad_in = recip * weighted - inputs * (recip * recip * recip) * inner_mean
    grad_gain = lax.optimization_barrier(jnp.sum(upstream * inputs * recip, axis=0))
    return (grad_in, grad_gain)

def group_norm(retained):
    centred = retained - lax.optimization_barrier(jnp.mean(retained, axis=-1, keepdims=True))
    inv_std = lax.rsqrt(lax.optimization_barrier(jnp.mean(centred * centred, axis=-1, keepdims=True)) + EPS)
    return (centred * inv_std, inv_std)

def group_norm_back(normed, inv_std, upstream):
    first_mean = lax.optimization_barrier(jnp.mean(upstream, axis=-1, keepdims=True))
    second_mean = lax.optimization_barrier(jnp.mean(upstream * normed, axis=-1, keepdims=True))
    return inv_std * (upstream - first_mean - normed * second_mean)

def silu_slope(inputs):
    sigmoid = jax.nn.sigmoid(inputs)
    return sigmoid * (1.0 + inputs * (1.0 - sigmoid))

def decay_tables(log_decay, rows):
    steps_in = jnp.arange(rows, dtype=jnp.float32)
    offset = steps_in[:, None] - steps_in[None, :]
    decay_mask = jnp.where(offset[None] >= 0.0, jnp.exp(log_decay[:, None, None] * jnp.maximum(offset, 0.0)[None]), 0.0)
    lead_decay = jnp.exp(log_decay[:, None] * (steps_in + 1.0))[:, :, None]
    tail_decay = jnp.exp(log_decay[:, None] * (rows - 1.0 - steps_in))[:, :, None]
    block_decay = jnp.exp(log_decay * rows)[:, None, None]
    return (decay_mask, lead_decay, tail_decay, block_decay)

def gelu_tanh(inputs):
    return jax.nn.gelu(inputs, approximate=True)

def rounded_f32(values):
    return lax.optimization_barrier(values.astype(jnp.bfloat16)).astype(jnp.float32)

def reference(layer_in, gain_one, w_query, w_key, w_value, w_gate, w_out, gain_two, w_ffgate, w_ffup, w_down, cotangent):
    rows = TOK_DEV
    blocks = TOKENS // rows
    per_seq = LENGTH // rows
    f32 = jnp.float32
    bf16 = jnp.bfloat16
    head_index = jnp.arange(HEADS).astype(f32)
    log_decay = jnp.log(1.0 - jnp.exp2(-5.0 - head_index))
    decay_mask, lead_decay, tail_decay, block_decay = decay_tables(log_decay, rows)
    cos_part, sin_part = rotation(jnp.arange(TOKENS) % LENGTH, DK // 2)
    scale = DK ** (-0.5)
    block_ids = jnp.arange(blocks)
    keep_fwd = (block_ids % per_seq != 0).astype(f32)
    keep_bwd = (block_ids % per_seq != per_seq - 1).astype(f32)

    def to_blocks(values, width):
        return values.reshape(blocks, rows, HEADS, width).transpose(0, 2, 1, 3)

    def from_blocks(values, width):
        return values.transpose(0, 2, 1, 3).reshape(TOKENS, HEADS, width)
    resid_in = layer_in.astype(f32)
    recip_one, normed_one = rms_forward(resid_in, gain_one)
    query = jnp.dot(normed_one, w_query, preferred_element_type=f32)
    key_proj = jnp.dot(normed_one, w_key, preferred_element_type=f32)
    gate_pre = jnp.dot(normed_one, w_gate, preferred_element_type=f32)
    value = jnp.dot(normed_one, w_value, preferred_element_type=f32).astype(bf16)
    query_rot = to_blocks((rotate(query.reshape(TOKENS, HEADS, DK), cos_part, sin_part) * scale).astype(bf16), DK)
    key_rot = to_blocks(rotate(key_proj.reshape(TOKENS, HEADS, DK), cos_part, sin_part).astype(bf16), DK)
    value_heads = to_blocks(value.reshape(TOKENS, HEADS, DV), DV)

    def local_state(items):
        key_dec = rounded_f32(items[0].astype(f32) * tail_decay)
        return jnp.einsum('hjd,hje->hde', key_dec, items[1].astype(f32), precision=PRECISE)
    local_states = lax.map(local_state, (key_rot, value_heads))

    def carry_step(carried, items):
        incoming, keep = items
        start = carried * keep
        return (block_decay * start + incoming, start)
    _, states_in = lax.scan(carry_step, jnp.zeros((HEADS, DK, DV), f32), (local_states, keep_fwd))

    def block_weights(query_b, key_b):
        scores = jnp.einsum('hid,hjd->hij', query_b.astype(f32), key_b.astype(f32))
        return (scores * decay_mask).astype(bf16)

    def stretch_forward(items):
        query_b, key_b, value_b, state_b = items
        weights_b = block_weights(query_b, key_b)
        intra = jnp.einsum('hij,hje->hie', weights_b.astype(f32), value_b.astype(f32))
        cross = jnp.einsum('hid,hde->hie', query_b.astype(f32), state_b, precision=PRECISE) * lead_decay
        return intra + cross
    retained = lax.map(stretch_forward, (query_rot, key_rot, value_heads, states_in))
    normed_heads, inv_std = group_norm(retained)
    normed_tok = from_blocks(normed_heads, DV).reshape(TOKENS, HEADS * DV)
    gate_act = jax.nn.silu(gate_pre)
    gated = (gate_act * normed_tok).astype(bf16)
    hidden_one = resid_in + jnp.dot(gated, w_out, preferred_element_type=f32)
    recip_two, normed_two = rms_forward(hidden_one, gain_two)
    ff_gate = jnp.dot(normed_two, w_ffgate, preferred_element_type=f32)
    ff_up = jnp.dot(normed_two, w_ffup, preferred_element_type=f32)
    ff_act, gelu_back = jax.vjp(gelu_tanh, ff_gate)
    inner_act = (ff_act * ff_up).astype(bf16)
    layer_out = (hidden_one + jnp.dot(inner_act, w_down, preferred_element_type=f32)).astype(bf16)
    upstream = cotangent.astype(f32)
    d_inner = jnp.dot(cotangent, w_down.T, preferred_element_type=f32)
    d_ffgate = gelu_back(d_inner * ff_up)[0].astype(bf16)
    d_ffup = (d_inner * ff_act).astype(bf16)
    grad_down = jnp.dot(inner_act.T, cotangent, preferred_element_type=f32)
    grad_ffgate = jnp.dot(normed_two.T, d_ffgate, preferred_element_type=f32)
    grad_ffup = jnp.dot(normed_two.T, d_ffup, preferred_element_type=f32)
    d_normtwo = jnp.dot(d_ffgate, w_ffgate.T, preferred_element_type=f32) + jnp.dot(d_ffup, w_ffup.T, preferred_element_type=f32)
    d_hidden_norm, grad_gain_two = rms_backward(hidden_one, recip_two, gain_two, d_normtwo)
    d_hidden = upstream + d_hidden_norm
    d_hidden_b = d_hidden.astype(bf16)
    grad_out = jnp.dot(gated.T, d_hidden_b, preferred_element_type=f32)
    d_gated = jnp.dot(d_hidden_b, w_out.T, preferred_element_type=f32)
    d_gatepre = (d_gated * normed_tok * silu_slope(gate_pre)).astype(bf16)
    d_normed = to_blocks(d_gated * gate_act, DV)
    d_ret_b = group_norm_back(normed_heads, inv_std, d_normed).astype(bf16)

    def state_grad(items):
        query_dec = rounded_f32(items[0].astype(f32) * lead_decay)
        return jnp.einsum('hid,hie->hde', query_dec, items[1].astype(f32), precision=PRECISE)
    d_states_in = lax.map(state_grad, (query_rot, d_ret_b))
    _, carried_back = lax.scan(carry_step, jnp.zeros((HEADS, DK, DV), f32), (d_states_in, keep_bwd), reverse=True)

    def stretch_backward(items):
        query_b, key_b, value_b, dret_b, state_b, back_b = items
        weights_b = block_weights(query_b, key_b)
        d_raw = jnp.einsum('hie,hje->hij', dret_b.astype(f32), value_b.astype(f32))
        d_weights = rounded_f32(d_raw * decay_mask)
        d_query = jnp.einsum('hij,hjd->hid', d_weights, key_b.astype(f32))
        d_query = d_query + jnp.einsum('hie,hde->hid', dret_b.astype(f32), state_b, precision=PRECISE) * lead_decay
        d_key = jnp.einsum('hij,hid->hjd', d_weights, query_b.astype(f32))
        d_key = d_key + jnp.einsum('hje,hde->hjd', value_b.astype(f32), back_b, precision=PRECISE) * tail_decay
        d_value = jnp.einsum('hij,hie->hje', weights_b.astype(f32), dret_b.astype(f32))
        d_value = d_value + jnp.einsum('hjd,hde->hje', key_b.astype(f32), back_b, precision=PRECISE) * tail_decay
        return (d_query, d_key, d_value)
    d_query, d_key, d_value = lax.map(stretch_backward, (query_rot, key_rot, value_heads, d_ret_b, states_in, carried_back))
    d_query_tok = (unrotate(from_blocks(d_query, DK), cos_part, sin_part) * scale).reshape(TOKENS, HEADS * DK).astype(bf16)
    d_key_tok = unrotate(from_blocks(d_key, DK), cos_part, sin_part).reshape(TOKENS, HEADS * DK).astype(bf16)
    d_value_tok = from_blocks(d_value, DV).reshape(TOKENS, HEADS * DV).astype(bf16)
    grad_query = jnp.dot(normed_one.T, d_query_tok, preferred_element_type=f32)
    grad_key = jnp.dot(normed_one.T, d_key_tok, preferred_element_type=f32)
    grad_value = jnp.dot(normed_one.T, d_value_tok, preferred_element_type=f32)
    grad_gate = jnp.dot(normed_one.T, d_gatepre, preferred_element_type=f32)
    d_normone = jnp.dot(d_query_tok, w_query.T, preferred_element_type=f32)
    d_normone = d_normone + jnp.dot(d_key_tok, w_key.T, preferred_element_type=f32)
    d_normone = d_normone + jnp.dot(d_value_tok, w_value.T, preferred_element_type=f32)
    d_normone = d_normone + jnp.dot(d_gatepre, w_gate.T, preferred_element_type=f32)
    d_input_norm, grad_gain_one = rms_backward(resid_in, recip_one, gain_one, d_normone)
    grad_input = d_hidden + d_input_norm
    return (layer_out, grad_input, grad_gain_one, grad_query, grad_key, grad_value, grad_gate, grad_out, grad_gain_two, grad_ffgate, grad_ffup, grad_down)
```

```python
import jax
import jax.numpy as jnp
from jax import lax
from jax.sharding import PartitionSpec as P

DK = 256
DV = 512
SEQS = 2

EPS = 1e-05
ROPE_BASE = 10000.0
F32 = jnp.float32
BF16 = jnp.bfloat16


def swap(value, axis, bit):
    count = lax.axis_size(axis)
    return lax.ppermute(value, axis, [(i, i ^ bit) for i in range(count)])


def rotation(positions, half_dim):
    frequency = ROPE_BASE ** (-jnp.arange(half_dim, dtype=F32) / half_dim)
    angles = positions.astype(F32)[:, None] * frequency[None, :]
    return (jnp.cos(angles), jnp.sin(angles))


def rotate(values, cos_part, sin_part):
    half_dim = cos_part.shape[1]
    leading = values[..., :half_dim]
    trailing = values[..., half_dim:]
    cos_wide = cos_part[:, None, :]
    sin_wide = sin_part[:, None, :]
    return jnp.concatenate(
        [leading * cos_wide - trailing * sin_wide, trailing * cos_wide + leading * sin_wide],
        axis=-1,
    )


def unrotate(gradient, cos_part, sin_part):
    half_dim = cos_part.shape[1]
    leading = gradient[..., :half_dim]
    trailing = gradient[..., half_dim:]
    return jnp.concatenate(
        [leading * cos_part + trailing * sin_part, trailing * cos_part - leading * sin_part],
        axis=-1,
    )


def group_norm(retained):
    centred = retained - jnp.mean(retained, axis=-1, keepdims=True)
    inv_std = lax.rsqrt(jnp.mean(centred * centred, axis=-1, keepdims=True) + EPS)
    return (centred * inv_std, inv_std)


def group_norm_back(normed, inv_std, upstream):
    first_mean = jnp.mean(upstream, axis=-1, keepdims=True)
    second_mean = jnp.mean(upstream * normed, axis=-1, keepdims=True)
    return inv_std * (upstream - first_mean - normed * second_mean)


def silu_slope(inputs):
    sigmoid = jax.nn.sigmoid(inputs)
    return sigmoid * (1.0 + inputs * (1.0 - sigmoid))


def rms_backward(inputs, recip, gain_vec, upstream):
    weighted = upstream * gain_vec
    inner_mean = jnp.mean(weighted * inputs, axis=-1, keepdims=True)
    grad_in = recip * weighted - inputs * (recip * recip * recip) * inner_mean
    grad_gain = jnp.sum(upstream * inputs * recip, axis=0)
    return (grad_in, grad_gain)


def decay_tables(log_decay, rows):
    steps_in = jnp.arange(rows, dtype=F32)
    offset = steps_in[:, None] - steps_in[None, :]
    decay_mask = jnp.where(
        offset[None] >= 0.0, jnp.exp(log_decay[:, None, None] * jnp.maximum(offset, 0.0)[None]), 0.0
    )
    lead_decay = jnp.exp(log_decay[:, None] * (steps_in + 1.0))[:, :, None]
    tail_decay = jnp.exp(log_decay[:, None] * (rows - 1.0 - steps_in))[:, :, None]
    return (decay_mask, lead_decay, tail_decay)


def gelu_tanh(inputs):
    return jax.nn.gelu(inputs, approximate=True)


def split_dot(lhs, rhs, spec):
    high = rhs.astype(BF16)
    low = (rhs - high.astype(F32)).astype(BF16)
    return jnp.einsum(spec, lhs, high, preferred_element_type=F32) + jnp.einsum(
        spec, lhs, low, preferred_element_type=F32
    )


def entering(state, log_decay, rows, place, per_seq):
    total = state
    carried = jnp.zeros_like(state)
    first = None
    bit = 1
    while bit < per_seq:
        other = swap(total, "seq", bit)
        if first is None:
            first = other
        upper = (place // bit) % 2 == 1
        reach = jnp.exp(log_decay * (rows * (place % bit)).astype(F32))[:, None, None]
        whole = jnp.exp(log_decay * float(rows * bit))[:, None, None]
        carried = carried + jnp.where(upper, reach * other, 0.0)
        if 2 * bit < per_seq:
            total = jnp.where(upper, whole * other + total, whole * total + other)
        bit *= 2
    return carried, first


def body(
    layer_in,
    gain_one,
    w_query,
    w_key,
    w_value,
    w_gate,
    w_out,
    gain_two,
    w_ffgate,
    w_ffup,
    w_down,
    cotangent,
):
    rows, width = layer_in.shape
    half = rows // 2
    heads_here = w_query.shape[1] // DK
    heads_half = heads_here // 2
    n_seq = lax.axis_size("seq")
    n_head = lax.axis_size("head")
    seq_at = lax.axis_index("seq")
    head_at = lax.axis_index("head")
    side = seq_at % 2
    core = head_at % 2
    lines = [list(range(k, n_seq, 2)) for k in range(2)]
    own_row = core * half
    oth_row = half - own_row

    def row_part(value, start):
        return lax.dynamic_slice_in_dim(value, start, half, axis=0)

    def natural(own, other):
        return jnp.concatenate(
            [jnp.where(core == 0, own, other), jnp.where(core == 0, other, own)], axis=0
        )

    def head_sum(send_rows, keep_rows):
        total = keep_rows + swap(send_rows, "head", 1)
        bit = 2
        while bit < n_head:
            total = total + swap(total, "head", bit)
            bit *= 2
        return total

    def dot(a, b):
        return jnp.dot(a, b, preferred_element_type=F32)

    def dot_t(a, b):
        return lax.dot_general(a, b, (((1,), (1,)), ((), ())), preferred_element_type=F32)

    def tdot(a, b):
        return lax.dot_general(a, b, (((0,), (0,)), ((), ())), preferred_element_type=F32)

    def line_scatter(partial):
        return lax.psum_scatter(
            partial, "seq", scatter_dimension=0, tiled=True, axis_index_groups=lines
        )

    def place_rows(reduced):
        mine = reduced.shape[0] // 2
        keep = lax.dynamic_slice_in_dim(reduced, side * mine, mine, axis=0)
        send = lax.dynamic_slice_in_dim(reduced, mine - side * mine, mine, axis=0)
        recv = swap(send, "seq", 1)
        return jnp.where(side == 0, keep, recv), jnp.where(side == 0, recv, keep)

    head_index = (head_at * heads_here + jnp.arange(heads_here)).astype(F32)
    log_decay = jnp.log(1.0 - jnp.exp2(-5.0 - head_index))
    decay_mask, lead_decay, tail_decay = decay_tables(log_decay, rows)
    per_seq = n_seq // SEQS
    place = seq_at % per_seq
    positions = place * rows + jnp.arange(rows)
    cos_part, sin_part = rotation(positions, DK // 2)
    scale = DK ** (-0.5)

    resid_in = layer_in.astype(F32)
    recip_one = lax.rsqrt(jnp.mean(resid_in * resid_in, axis=-1, keepdims=True) + EPS)
    scaled_one = resid_in * recip_one
    normed_one = (scaled_one * gain_one).astype(BF16)
    key_proj = dot(normed_one, w_key)
    value = dot(normed_one, w_value).astype(BF16)
    key_rot = (
        rotate(key_proj.reshape(rows, heads_here, DK), cos_part, sin_part)
        .astype(BF16)
        .transpose(1, 0, 2)
    )
    value_heads = value.reshape(rows, heads_here, DV).transpose(1, 0, 2)
    key_dec = (key_rot.astype(F32) * tail_decay).astype(BF16)
    local_state = jnp.einsum("hjd,hje->hde", key_dec, value_heads, preferred_element_type=F32)
    state_in, state_got = entering(local_state, log_decay, rows, place, per_seq)

    one_send, cot_send, _ = lax.optimization_barrier(
        (
            row_part(resid_in, own_row) * row_part(recip_one, own_row),
            row_part(cotangent, own_row).astype(F32) * 0.5,
            state_got,
        )
    )
    one_own = swap(one_send, "seq", 1)
    one_oth = swap(one_own, "head", 1)
    normed_one_y = (natural(one_own, one_oth) * gain_one).astype(BF16)
    cot_own_y = swap(cot_send, "seq", 1)
    cot_oth_y = swap(cot_own_y, "head", 1)

    query = dot(normed_one, w_query)
    gate_pre = dot(normed_one, w_gate)
    query_rot = (
        (rotate(query.reshape(rows, heads_here, DK), cos_part, sin_part) * scale)
        .astype(BF16)
        .transpose(1, 0, 2)
    )
    scores = jnp.einsum("hid,hjd->hij", query_rot, key_rot, preferred_element_type=F32)
    weights_b = (scores * decay_mask).astype(BF16)
    retained = jnp.einsum("hij,hje->hie", weights_b, value_heads, preferred_element_type=F32)
    retained = retained + split_dot(query_rot, state_in, "hid,hde->hie") * lead_decay
    normed_heads, inv_std = group_norm(retained)
    normed_tok = normed_heads.transpose(1, 0, 2).reshape(rows, heads_here * DV)
    gate_act = jax.nn.silu(gate_pre)
    gated = (gate_act * normed_tok).astype(BF16)

    mix_send = dot(row_part(gated, oth_row), w_out)
    mix_keep = dot(row_part(gated, own_row), w_out)
    resid_own = row_part(layer_in, own_row).astype(F32)
    hidden_own = resid_own + head_sum(mix_send, mix_keep)
    recip_two = lax.rsqrt(jnp.mean(hidden_own * hidden_own, axis=-1, keepdims=True) + EPS)
    two_own = hidden_own * recip_two
    two_oth = swap(two_own, "head", 1)
    normed_two = (jnp.concatenate([two_own, two_oth], axis=0) * gain_two).astype(BF16)

    cot_own = row_part(cotangent, own_row)
    cot_oth = row_part(cotangent, oth_row)
    cot_perm = jnp.concatenate([cot_own, cot_oth], axis=0)
    d_inner = dot_t(cot_perm, w_down)
    ff_gate = dot(normed_two, w_ffgate)
    ff_up = dot(normed_two, w_ffup)
    ff_act, gelu_back = jax.vjp(gelu_tanh, ff_gate)
    inner_act = (ff_act * ff_up).astype(BF16)
    d_ffgate_f = gelu_back(d_inner * ff_up)[0]
    d_ffup_f = d_inner * ff_act
    d_ffgate = d_ffgate_f.astype(BF16)
    d_ffup = d_ffup_f.astype(BF16)

    def two_part(gate_rows, up_rows):
        return dot_t(gate_rows, w_ffgate) + dot_t(up_rows, w_ffup)

    two_send = two_part(d_ffgate[half:], d_ffup[half:])
    two_keep = two_part(d_ffgate[:half], d_ffup[:half])
    d_normtwo = head_sum(two_send, two_keep)

    two_own_y = swap(two_own, "seq", 1)
    two_oth_y = swap(two_own_y, "head", 1)
    normed_two_y = (jnp.concatenate([two_own_y, two_oth_y], axis=0) * gain_two).astype(BF16)
    cot_perm_y = (jnp.concatenate([cot_own_y, cot_oth_y], axis=0) * 2.0).astype(BF16)

    ff_half = inner_act.shape[1] // 2
    inner_f = ff_act * ff_up
    inner_send = jnp.where(side == 0, inner_f[:, ff_half:], inner_f[:, :ff_half]) * 0.5
    inner_keep = jnp.where(side == 0, inner_act[:, :ff_half], inner_act[:, ff_half:])
    inner_recv = (swap(inner_send, "seq", 1) * 2.0).astype(BF16)
    red_down = line_scatter(tdot(cot_perm, inner_keep) + tdot(cot_perm_y, inner_recv))

    dff_send = jnp.where(side == 0, d_ffup_f, d_ffgate_f) * 0.5
    dff_keep = jnp.where(side == 0, d_ffgate, d_ffup)
    dff_recv = (swap(dff_send, "seq", 1) * 2.0).astype(BF16)
    red_ff = line_scatter(tdot(normed_two, dff_keep) + tdot(normed_two_y, dff_recv))

    d_hidden_norm, gain_two_part = rms_backward(hidden_own, recip_two, gain_two, d_normtwo)
    dhn_oth = swap(d_hidden_norm, "head", 1)
    d_hidden_own = cot_own.astype(F32) + d_hidden_norm
    d_hidden_b = natural(d_hidden_own, cot_oth.astype(F32) + dhn_oth).astype(BF16)

    ffn_send = dot(inner_act[half:], w_down)
    ffn_keep = dot(inner_act[:half], w_down)
    out_own = hidden_own + head_sum(ffn_send, ffn_keep)
    out_oth = swap(out_own * 0.5, "head", 1) * 2.0
    layer_out = natural(out_own, out_oth).astype(BF16)

    d_gated = dot_t(d_hidden_b, w_out)
    d_gatepre_f = d_gated * normed_tok * silu_slope(gate_pre)
    d_gatepre = d_gatepre_f.astype(BF16)
    d_normed = (d_gated * gate_act).reshape(rows, heads_here, DV).transpose(1, 0, 2)
    d_ret_b = group_norm_back(normed_heads, inv_std, d_normed).astype(BF16)
    query_dec = (query_rot.astype(F32) * lead_decay).astype(BF16)
    d_state = jnp.einsum("hid,hie->hde", query_dec, d_ret_b, preferred_element_type=F32)
    carried_back, back_got = entering(d_state, log_decay, rows, per_seq - 1 - place, per_seq)

    dhn_send, _ = lax.optimization_barrier((d_hidden_norm, back_got))
    dhn_own_y = swap(dhn_send, "seq", 1)
    dhn_oth_y = swap(dhn_own_y, "head", 1)
    d_hidden_b_y = natural(
        cot_own_y * 2.0 + dhn_own_y, cot_oth_y * 2.0 + dhn_oth_y
    ).astype(BF16)

    wide = heads_half * DV

    def cols(value, which):
        return lax.dynamic_slice_in_dim(value, which * wide, wide, axis=1)

    gated_f = gate_act * normed_tok
    gated_recv = (swap(cols(gated_f, 1 - side) * 0.5, "seq", 1) * 2.0).astype(BF16)
    gate_recv = (swap(cols(d_gatepre_f, 1 - side) * 0.5, "seq", 1) * 2.0).astype(BF16)
    red_gate = line_scatter(
        tdot(normed_one, cols(d_gatepre, side)) + tdot(normed_one_y, gate_recv)
    )
    red_out = line_scatter(
        tdot(d_hidden_b, cols(gated, side)) + tdot(d_hidden_b_y, gated_recv)
    )

    d_raw = jnp.einsum("hie,hje->hij", d_ret_b, value_heads, preferred_element_type=F32)
    d_weights = (d_raw * decay_mask).astype(BF16)
    d_query = jnp.einsum("hij,hjd->hid", d_weights, key_rot, preferred_element_type=F32)
    d_query = d_query + split_dot(d_ret_b, state_in, "hie,hde->hid") * lead_decay
    d_key = jnp.einsum("hij,hid->hjd", d_weights, query_rot, preferred_element_type=F32)
    d_key = d_key + split_dot(value_heads, carried_back, "hje,hde->hjd") * tail_decay
    d_value = jnp.einsum("hij,hie->hje", weights_b, d_ret_b, preferred_element_type=F32)
    d_value = d_value + split_dot(key_rot, carried_back, "hjd,hde->hje") * tail_decay
    d_query = unrotate(d_query, cos_part, sin_part) * scale
    d_key = unrotate(d_key, cos_part, sin_part)
    d_query_b, d_key_b, d_value_b = (v.astype(BF16) for v in (d_query, d_key, d_value))

    def tokens(value):
        return value.transpose(1, 0, 2).reshape(rows, -1)

    def head_half(value, which):
        part = lax.dynamic_slice_in_dim(value, which * heads_half, heads_half, axis=0)
        return tokens(part)

    qkv_send = jnp.concatenate([head_half(v, 1 - side) for v in (d_query, d_key, d_value)], axis=1)
    qkv_keep = jnp.concatenate(
        [head_half(v, side) for v in (d_query_b, d_key_b, d_value_b)], axis=1
    )
    qkv_recv = (swap(qkv_send * 0.5, "seq", 1) * 2.0).astype(BF16)
    red_qkv = line_scatter(tdot(normed_one, qkv_keep) + tdot(normed_one_y, qkv_recv))

    dq_tok, dk_tok, dv_tok = tokens(d_query_b), tokens(d_key_b), tokens(d_value_b)

    def one_part(start):
        return (
            dot_t(row_part(dq_tok, start), w_query)
            + dot_t(row_part(dk_tok, start), w_key)
            + dot_t(row_part(dv_tok, start), w_value)
            + dot_t(row_part(d_gatepre, start), w_gate)
        )

    d_normone = head_sum(one_part(oth_row), one_part(own_row))
    d_input_norm, gain_one_part = rms_backward(
        resid_own, row_part(recip_one, own_row), gain_one, d_normone
    )
    grad_own = d_hidden_own + d_input_norm
    grad_input = natural(grad_own, swap(grad_own, "head", 1))

    gains = jnp.stack([gain_one_part, gain_two_part]) * (2.0 / n_head)
    gains = lax.psum(gains, ("seq", "head"))
    chunk = width // n_seq
    gains = lax.dynamic_slice_in_dim(gains, seq_at * chunk, chunk, axis=1)

    down_lo, down_hi = place_rows(red_down)
    grad_down = jnp.concatenate([down_lo, down_hi], axis=1).T
    grad_ffgate, grad_ffup = place_rows(red_ff)
    grad_gate = jnp.concatenate(place_rows(red_gate), axis=1)
    grad_out = jnp.concatenate(place_rows(red_out), axis=1).T
    qkv_lo, qkv_hi = place_rows(red_qkv)
    kw = heads_half * DK
    grad_query = jnp.concatenate([qkv_lo[:, :kw], qkv_hi[:, :kw]], axis=1)
    grad_key = jnp.concatenate([qkv_lo[:, kw : 2 * kw], qkv_hi[:, kw : 2 * kw]], axis=1)
    grad_value = jnp.concatenate([qkv_lo[:, 2 * kw :], qkv_hi[:, 2 * kw :]], axis=1)
    return (
        layer_out,
        grad_input,
        gains[0],
        grad_query,
        grad_key,
        grad_value,
        grad_gate,
        grad_out,
        gains[1],
        grad_ffgate,
        grad_ffup,
        grad_down,
    )


def solution(mesh):
    in_specs = (
        P("seq", None),
        P(),
        P(None, "head"),
        P(None, "head"),
        P(None, "head"),
        P(None, "head"),
        P("head", None),
        P(),
        P(None, "head"),
        P(None, "head"),
        P("head", None),
        P("seq", None),
    )
    out_specs = (
        P("seq", None),
        P("seq", None),
        P("seq"),
        P("seq", "head"),
        P("seq", "head"),
        P("seq", "head"),
        P("seq", "head"),
        P("head", "seq"),
        P("seq"),
        P("seq", "head"),
        P("seq", "head"),
        P("head", "seq"),
    )
    return jax.shard_map(body, mesh=mesh, in_specs=in_specs, out_specs=out_specs, check_vma=False)
```

```python
import jax
import jax.numpy as jnp
from jax import lax
from jax.sharding import PartitionSpec as P


DK = 256
DV = 512
SEQS = 2

EPS = 1e-05
ROPE_BASE = 10000.0
F32 = jnp.float32
BF16 = jnp.bfloat16


def swap(value, axis, bit):
    count = lax.axis_size(axis)
    return lax.ppermute(value, axis, [(i, i ^ bit) for i in range(count)])


def rotation(positions, half_dim):
    frequency = ROPE_BASE ** (-jnp.arange(half_dim, dtype=F32) / half_dim)
    angles = positions.astype(F32)[:, None] * frequency[None, :]
    return (jnp.cos(angles), jnp.sin(angles))


def rotate(values, cos_part, sin_part):
    half_dim = cos_part.shape[1]
    leading = values[..., :half_dim]
    trailing = values[..., half_dim:]
    cos_wide = cos_part[:, None, :]
    sin_wide = sin_part[:, None, :]
    return jnp.concatenate(
        [leading * cos_wide - trailing * sin_wide, trailing * cos_wide + leading * sin_wide],
        axis=-1,
    )


def unrotate(gradient, cos_part, sin_part):
    half_dim = cos_part.shape[1]
    leading = gradient[..., :half_dim]
    trailing = gradient[..., half_dim:]
    return jnp.concatenate(
        [leading * cos_part + trailing * sin_part, trailing * cos_part - leading * sin_part],
        axis=-1,
    )


def group_norm(retained):
    centred = retained - jnp.mean(retained, axis=-1, keepdims=True)
    inv_std = lax.rsqrt(jnp.mean(centred * centred, axis=-1, keepdims=True) + EPS)
    return (centred * inv_std, inv_std)


def group_norm_back(normed, inv_std, upstream):
    first_mean = jnp.mean(upstream, axis=-1, keepdims=True)
    second_mean = jnp.mean(upstream * normed, axis=-1, keepdims=True)
    return inv_std * (upstream - first_mean - normed * second_mean)


def silu_slope(inputs):
    sigmoid = jax.nn.sigmoid(inputs)
    return sigmoid * (1.0 + inputs * (1.0 - sigmoid))


def rms_backward(inputs, recip, gain_vec, upstream):
    weighted = upstream * gain_vec
    inner_mean = jnp.mean(weighted * inputs, axis=-1, keepdims=True)
    grad_in = recip * weighted - inputs * (recip * recip * recip) * inner_mean
    grad_gain = jnp.sum(upstream * inputs * recip, axis=0)
    return (grad_in, grad_gain)


def decay_tables(log_decay, rows):
    steps_in = jnp.arange(rows, dtype=F32)
    offset = steps_in[:, None] - steps_in[None, :]
    decay_mask = jnp.where(
        offset[None] >= 0.0, jnp.exp(log_decay[:, None, None] * jnp.maximum(offset, 0.0)[None]), 0.0
    )
    lead_decay = jnp.exp(log_decay[:, None] * (steps_in + 1.0))[:, :, None]
    tail_decay = jnp.exp(log_decay[:, None] * (rows - 1.0 - steps_in))[:, :, None]
    return (decay_mask, lead_decay, tail_decay)


def gelu_tanh(inputs):
    return jax.nn.gelu(inputs, approximate=True)


def split_dot(lhs, rhs, spec):
    high = rhs.astype(BF16)
    low = (rhs - high.astype(F32)).astype(BF16)
    return jnp.einsum(spec, lhs, high, preferred_element_type=F32) + jnp.einsum(
        spec, lhs, low, preferred_element_type=F32
    )


def entering(state, log_decay, rows, place, per_seq):
    total = state
    carried = jnp.zeros_like(state)
    bit = 1
    while bit < per_seq:
        other = swap(total, "seq", bit)
        upper = (place // bit) % 2 == 1
        reach = jnp.exp(log_decay * (rows * (place % bit)).astype(F32))[:, None, None]
        whole = jnp.exp(log_decay * float(rows * bit))[:, None, None]
        carried = carried + jnp.where(upper, reach * other, 0.0)
        if 2 * bit < per_seq:
            total = jnp.where(upper, whole * other + total, whole * total + other)
        bit *= 2
    return carried


def compute(
    layer_in,
    gain_one,
    w_query,
    w_key,
    w_value,
    w_gate,
    w_out,
    gain_two,
    w_ffgate,
    w_ffup,
    w_down,
    cotangent,
):
    rows, width = layer_in.shape
    half = rows // 2
    heads_here = w_query.shape[1] // DK
    heads_half = heads_here // 2
    n_seq = lax.axis_size("seq")
    n_head = lax.axis_size("head")
    seq_at = lax.axis_index("seq")
    head_at = lax.axis_index("head")
    side = seq_at % 2
    core = head_at % 2
    lines = [list(range(k, n_seq, 2)) for k in range(2)]
    own_row = core * half
    oth_row = half - own_row

    def row_part(value, start):
        return lax.dynamic_slice_in_dim(value, start, half, axis=0)

    def natural(own, other):
        return jnp.concatenate(
            [jnp.where(core == 0, own, other), jnp.where(core == 0, other, own)], axis=0
        )

    def head_sum(send_rows, keep_rows):
        total = keep_rows + swap(send_rows, "head", 1)
        bit = 2
        while bit < n_head:
            total = total + swap(total, "head", bit)
            bit *= 2
        return total

    def contract(a, b, dims):
        return lax.dot_general(a, b, (dims, ((), ())), preferred_element_type=F32)

    def dot(a, b):
        return contract(a, b, ((1,), (0,)))

    def dot_t(a, b):
        return contract(a, b, ((1,), (1,)))

    def tdot(a, b):
        return contract(a, b, ((0,), (0,)))

    def line_scatter(partial):
        return lax.psum_scatter(
            partial, "seq", scatter_dimension=0, tiled=True, axis_index_groups=lines
        )

    def place_rows(reduced):
        mine = reduced.shape[0] // 2
        keep = lax.dynamic_slice_in_dim(reduced, side * mine, mine, axis=0)
        send = lax.dynamic_slice_in_dim(reduced, mine - side * mine, mine, axis=0)
        recv = swap(send, "seq", 1)
        return jnp.where(side == 0, keep, recv), jnp.where(side == 0, recv, keep)

    head_index = (head_at * heads_here + jnp.arange(heads_here)).astype(F32)
    log_decay = jnp.log(1.0 - jnp.exp2(-5.0 - head_index))
    decay_mask, lead_decay, tail_decay = decay_tables(log_decay, rows)
    per_seq = n_seq // SEQS
    place = seq_at % per_seq
    positions = place * rows + jnp.arange(rows)
    cos_part, sin_part = rotation(positions, DK // 2)
    scale = DK ** (-0.5)

    resid_in = layer_in.astype(F32)
    recip_one = lax.rsqrt(jnp.mean(resid_in * resid_in, axis=-1, keepdims=True) + EPS)
    scaled_one = resid_in * recip_one
    normed_one = (scaled_one * gain_one).astype(BF16)
    key_proj = dot(normed_one, w_key)
    value = dot(normed_one, w_value).astype(BF16)
    key_rot = (
        rotate(key_proj.reshape(rows, heads_here, DK), cos_part, sin_part)
        .astype(BF16)
        .transpose(1, 0, 2)
    )
    value_heads = value.reshape(rows, heads_here, DV).transpose(1, 0, 2)
    key_dec = (key_rot.astype(F32) * tail_decay).astype(BF16)
    local_state = jnp.einsum("hjd,hje->hde", key_dec, value_heads, preferred_element_type=F32)
    state_in = entering(local_state, log_decay, rows, place, per_seq)

    late_in, late_cot, late_one, late_recip, _ = lax.optimization_barrier(
        (layer_in, cotangent, normed_one, recip_one, local_state)
    )
    one_send = row_part(late_in, own_row).astype(F32) * row_part(late_recip, own_row)
    cot_send = row_part(late_cot, own_row).astype(F32) * 0.5
    one_own = swap(one_send, "seq", 1)
    one_oth = swap(one_own, "head", 1)
    normed_one_y = (natural(one_own, one_oth) * gain_one).astype(BF16)
    cot_own_y = swap(cot_send, "seq", 1)
    cot_oth_y = swap(cot_own_y, "head", 1)

    query = dot(late_one, w_query)
    gate_pre = lax.optimization_barrier(dot(late_one, w_gate))
    query_rot = (
        (rotate(query.reshape(rows, heads_here, DK), cos_part, sin_part) * scale)
        .astype(BF16)
        .transpose(1, 0, 2)
    )
    scores = jnp.einsum("hid,hjd->hij", query_rot, key_rot, preferred_element_type=F32)
    weights_b = (scores * decay_mask).astype(BF16)
    retained = jnp.einsum("hij,hje->hie", weights_b, value_heads, preferred_element_type=F32)
    retained = lax.optimization_barrier(retained)
    retained = retained + split_dot(query_rot, state_in, "hid,hde->hie") * lead_decay
    normed_heads, inv_std = group_norm(retained)
    normed_tok = normed_heads.transpose(1, 0, 2).reshape(rows, heads_here * DV)
    gate_act = jax.nn.silu(gate_pre)
    gated = (gate_act * normed_tok).astype(BF16)

    mix_send = dot(row_part(gated, oth_row), w_out)
    mix_keep = dot(row_part(gated, own_row), w_out)
    resid_own = row_part(layer_in, own_row).astype(F32)
    hidden_own = resid_own + head_sum(mix_send, mix_keep)
    recip_two = lax.rsqrt(jnp.mean(hidden_own * hidden_own, axis=-1, keepdims=True) + EPS)
    two_own = hidden_own * recip_two
    two_oth = swap(two_own, "head", 1)
    normed_two = (jnp.concatenate([two_own, two_oth], axis=0) * gain_two).astype(BF16)

    cot_own = row_part(cotangent, own_row)
    cot_oth = row_part(cotangent, oth_row)
    cot_perm = jnp.concatenate([cot_own, cot_oth], axis=0)
    d_inner = dot_t(cot_perm, w_down)
    ff_gate = dot(normed_two, w_ffgate)
    ff_up = dot(normed_two, w_ffup)
    ff_act, gelu_back = jax.vjp(gelu_tanh, ff_gate)
    inner_act = (ff_act * ff_up).astype(BF16)
    d_ffgate_f = gelu_back(d_inner * ff_up)[0]
    d_ffup_f = d_inner * ff_act
    d_ffgate = d_ffgate_f.astype(BF16)
    d_ffup = d_ffup_f.astype(BF16)

    def two_part(gate_rows, up_rows):
        return dot_t(gate_rows, w_ffgate) + dot_t(up_rows, w_ffup)

    two_send = two_part(d_ffgate[half:], d_ffup[half:])
    two_keep = two_part(d_ffgate[:half], d_ffup[:half])
    d_normtwo = head_sum(two_send, two_keep)

    across = (head_at // 2) % 2
    if n_head % 4 == 0:
        span = width // 2
        two_piece = lax.dynamic_slice_in_dim(two_own, across * span, span, axis=1)
        two_piece_y = swap(two_piece, "seq", 1)
        two_piece_x = swap(two_piece_y, "head", 2)
        two_own_y = jnp.concatenate(
            [
                jnp.where(across == 0, two_piece_y, two_piece_x),
                jnp.where(across == 0, two_piece_x, two_piece_y),
            ],
            axis=1,
        )
    else:
        two_own_y = swap(two_own, "seq", 1)
    two_oth_y = swap(two_own_y, "head", 1)
    normed_two_y = (jnp.concatenate([two_own_y, two_oth_y], axis=0) * gain_two).astype(BF16)
    cot_perm_y = (jnp.concatenate([cot_own_y, cot_oth_y], axis=0) * 2.0).astype(BF16)

    ff_half = inner_act.shape[1] // 2
    inner_f = ff_act * ff_up
    inner_send = jnp.where(side == 0, inner_f[:, ff_half:], inner_f[:, :ff_half]) * 0.5
    inner_keep = jnp.where(side == 0, inner_act[:, :ff_half], inner_act[:, ff_half:])
    inner_recv = (swap(inner_send, "seq", 1) * 2.0).astype(BF16)
    red_down = line_scatter(tdot(cot_perm, inner_keep) + tdot(cot_perm_y, inner_recv))

    dff_send = jnp.where(side == 0, d_ffup_f, d_ffgate_f) * 0.5
    dff_keep = jnp.where(side == 0, d_ffgate, d_ffup)
    dff_recv = (swap(dff_send, "seq", 1) * 2.0).astype(BF16)
    red_ff = line_scatter(tdot(normed_two, dff_keep) + tdot(normed_two_y, dff_recv))

    d_hidden_norm, gain_two_part = rms_backward(hidden_own, recip_two, gain_two, d_normtwo)
    dhn_oth = swap(d_hidden_norm, "head", 1)
    d_hidden_own = cot_own.astype(F32) + d_hidden_norm
    d_hidden_b = natural(d_hidden_own, cot_oth.astype(F32) + dhn_oth).astype(BF16)

    ffn_send = dot(inner_act[half:], w_down)
    ffn_keep = dot(inner_act[:half], w_down)
    ffn_sum = head_sum(ffn_send, ffn_keep)

    d_gated = dot_t(d_hidden_b, w_out)
    d_gatepre_f = d_gated * normed_tok * silu_slope(gate_pre)
    d_normed = (d_gated * gate_act).reshape(rows, heads_here, DV).transpose(1, 0, 2)
    d_ret_b = group_norm_back(normed_heads, inv_std, d_normed).astype(BF16)
    late_hidden, d_ret_b, late_pre = lax.optimization_barrier((hidden_own, d_ret_b, d_gatepre_f))
    d_gatepre = late_pre.astype(BF16)
    out_own = late_hidden + ffn_sum
    out_oth = swap(out_own * 0.5, "head", 1) * 2.0
    layer_out = natural(out_own, out_oth).astype(BF16)
    query_dec = (query_rot.astype(F32) * lead_decay).astype(BF16)
    d_state = jnp.einsum("hid,hie->hde", query_dec, d_ret_b, preferred_element_type=F32)
    carried_back = entering(d_state, log_decay, rows, per_seq - 1 - place, per_seq)

    dhn_send = d_hidden_norm
    dhn_own_y = swap(dhn_send, "seq", 1)
    dhn_oth_y = swap(dhn_own_y, "head", 1)
    d_hidden_b_y = natural(
        cot_own_y * 2.0 + dhn_own_y, cot_oth_y * 2.0 + dhn_oth_y
    ).astype(BF16)

    wide = heads_half * DV

    def cols(value, which):
        return lax.dynamic_slice_in_dim(value, which * wide, wide, axis=1)

    gated_f = gate_act * normed_tok
    gated_recv = (swap(cols(gated_f, 1 - side) * 0.5, "seq", 1) * 2.0).astype(BF16)
    gate_recv = (swap(cols(late_pre, 1 - side) * 0.5, "seq", 1) * 2.0).astype(BF16)
    red_gate = line_scatter(tdot(normed_one, cols(d_gatepre, side)) + tdot(normed_one_y, gate_recv))
    red_out = line_scatter(tdot(d_hidden_b, cols(gated, side)) + tdot(d_hidden_b_y, gated_recv))

    d_raw = jnp.einsum("hie,hje->hij", d_ret_b, value_heads, preferred_element_type=F32)
    d_weights = (d_raw * decay_mask).astype(BF16)
    d_query = jnp.einsum("hij,hjd->hid", d_weights, key_rot, preferred_element_type=F32)
    d_query = d_query + split_dot(d_ret_b, state_in, "hie,hde->hid") * lead_decay
    d_key = jnp.einsum("hij,hid->hjd", d_weights, query_rot, preferred_element_type=F32)
    d_key = d_key + split_dot(value_heads, carried_back, "hje,hde->hjd") * tail_decay
    d_value = jnp.einsum("hij,hie->hje", weights_b, d_ret_b, preferred_element_type=F32)
    d_value = d_value + split_dot(key_rot, carried_back, "hjd,hde->hje") * tail_decay
    d_query = unrotate(d_query, cos_part, sin_part) * scale
    d_key = unrotate(d_key, cos_part, sin_part)
    d_query_b, d_key_b, d_value_b = (v.astype(BF16) for v in (d_query, d_key, d_value))

    def tokens(value):
        return value.transpose(1, 0, 2).reshape(rows, -1)

    def head_half(value, which):
        part = lax.dynamic_slice_in_dim(value, which * heads_half, heads_half, axis=0)
        return tokens(part)

    qkv_send = jnp.concatenate([head_half(v, 1 - side) for v in (d_value, d_query, d_key)], axis=1)
    qkv_recv = (swap(qkv_send * 0.5, "seq", 1) * 2.0).astype(BF16)
    qk_keep = jnp.concatenate([head_half(v, side) for v in (d_query_b, d_key_b)], axis=1)
    red_v = line_scatter(
        tdot(normed_one, head_half(d_value_b, side)) + tdot(normed_one_y, qkv_recv[:, :wide])
    )
    red_qk = line_scatter(tdot(normed_one, qk_keep) + tdot(normed_one_y, qkv_recv[:, wide:]))

    dq_tok, dk_tok, dv_tok = tokens(d_query_b), tokens(d_key_b), tokens(d_value_b)

    def one_part(start):
        return (
            dot_t(row_part(dq_tok, start), w_query)
            + dot_t(row_part(dk_tok, start), w_key)
            + dot_t(row_part(d_gatepre, start), w_gate)
            + dot_t(row_part(dv_tok, start), w_value)
        )

    d_normone = head_sum(one_part(oth_row), one_part(own_row))
    d_input_norm, gain_one_part = rms_backward(
        resid_own, row_part(recip_one, own_row), gain_one, d_normone
    )
    grad_own = d_hidden_own + d_input_norm
    grad_input = natural(grad_own, swap(grad_own, "head", 1))

    gains = jnp.stack([gain_one_part, gain_two_part])
    gains = gains + swap(gains, "head", 1)
    bit = 1
    while bit < n_seq:
        gains = gains + swap(gains, "seq", bit)
        bit *= 2
    chunk = width // n_seq
    gains = lax.dynamic_slice_in_dim(gains, seq_at * chunk, chunk, axis=1)

    down_lo, down_hi = place_rows(red_down)
    grad_down = jnp.concatenate([down_lo, down_hi], axis=1).T
    grad_ffgate, grad_ffup = place_rows(red_ff)
    grad_gate = jnp.concatenate(place_rows(red_gate), axis=1)
    grad_out = jnp.concatenate(place_rows(red_out), axis=1).T
    grad_value = jnp.concatenate(place_rows(red_v), axis=1)
    qk_lo, qk_hi = place_rows(red_qk)
    kw = heads_half * DK
    grad_query = jnp.concatenate([qk_lo[:, :kw], qk_hi[:, :kw]], axis=1)
    grad_key = jnp.concatenate([qk_lo[:, kw:], qk_hi[:, kw:]], axis=1)
    return (
        layer_out,
        grad_input,
        gains[0],
        grad_query,
        grad_key,
        grad_value,
        grad_gate,
        grad_out,
        gains[1],
        grad_ffgate,
        grad_ffup,
        grad_down,
    )


def solution(mesh):
    in_specs = (
        P("seq", None),
        P(),
        P(None, "head"),
        P(None, "head"),
        P(None, "head"),
        P(None, "head"),
        P("head", None),
        P(),
        P(None, "head"),
        P(None, "head"),
        P("head", None),
        P("seq", None),
    )
    out_specs = (
        P("seq", None),
        P("seq", None),
        P("seq"),
        P("seq", "head"),
        P("seq", "head"),
        P("seq", "head"),
        P("seq", "head"),
        P("head", "seq"),
        P("seq"),
        P("seq", "head"),
        P("seq", "head"),
        P("head", "seq"),
    )
    return jax.shard_map(compute, mesh=mesh, in_specs=in_specs, out_specs=out_specs, check_vma=False)
```

```python
import jax
import jax.numpy as jnp
from jax import lax
from jax.sharding import PartitionSpec as P


DK = 256
DV = 512
SEQS = 2

EPS = 1e-05
ROPE_BASE = 10000.0
F32 = jnp.float32
BF16 = jnp.bfloat16


def swap(value, axis, bit):
    count = lax.axis_size(axis)
    return lax.ppermute(value, axis, [(i, i ^ bit) for i in range(count)])


def rotation(positions, half_dim):
    frequency = ROPE_BASE ** (-jnp.arange(half_dim, dtype=F32) / half_dim)
    angles = positions.astype(F32)[:, None] * frequency[None, :]
    return (jnp.cos(angles), jnp.sin(angles))


def rotate(values, cos_part, sin_part):
    half_dim = cos_part.shape[1]
    leading = values[..., :half_dim]
    trailing = values[..., half_dim:]
    cos_wide = cos_part[:, None, :]
    sin_wide = sin_part[:, None, :]
    return jnp.concatenate(
        [leading * cos_wide - trailing * sin_wide, trailing * cos_wide + leading * sin_wide],
        axis=-1,
    )


def unrotate(gradient, cos_part, sin_part):
    half_dim = cos_part.shape[1]
    leading = gradient[..., :half_dim]
    trailing = gradient[..., half_dim:]
    return jnp.concatenate(
        [leading * cos_part + trailing * sin_part, trailing * cos_part - leading * sin_part],
        axis=-1,
    )


def group_norm(retained):
    centred = retained - jnp.mean(retained, axis=-1, keepdims=True)
    inv_std = lax.rsqrt(jnp.mean(centred * centred, axis=-1, keepdims=True) + EPS)
    return (centred * inv_std, inv_std)


def group_norm_back(normed, inv_std, upstream):
    first_mean = jnp.mean(upstream, axis=-1, keepdims=True)
    second_mean = jnp.mean(upstream * normed, axis=-1, keepdims=True)
    return inv_std * (upstream - first_mean - normed * second_mean)


def silu_slope(inputs):
    sigmoid = jax.nn.sigmoid(inputs)
    return sigmoid * (1.0 + inputs * (1.0 - sigmoid))


def rms_backward(inputs, recip, gain_vec, upstream):
    weighted = upstream * gain_vec
    inner_mean = jnp.mean(weighted * inputs, axis=-1, keepdims=True)
    grad_in = recip * weighted - inputs * (recip * recip * recip) * inner_mean
    grad_gain = jnp.sum(upstream * inputs * recip, axis=0)
    return (grad_in, grad_gain)


def decay_tables(log_decay, rows):
    steps_in = jnp.arange(rows, dtype=F32)
    offset = steps_in[:, None] - steps_in[None, :]
    decay_mask = jnp.where(
        offset[None] >= 0.0, jnp.exp(log_decay[:, None, None] * jnp.maximum(offset, 0.0)[None]), 0.0
    )
    lead_decay = jnp.exp(log_decay[:, None] * (steps_in + 1.0))[:, :, None]
    tail_decay = jnp.exp(log_decay[:, None] * (rows - 1.0 - steps_in))[:, :, None]
    return (decay_mask, lead_decay, tail_decay)


def gelu_tanh(inputs):
    return jax.nn.gelu(inputs, approximate=True)


def split_dot(lhs, rhs, spec):
    high = rhs.astype(BF16)
    low = (rhs - high.astype(F32)).astype(BF16)
    return jnp.einsum(spec, lhs, high, preferred_element_type=F32) + jnp.einsum(
        spec, lhs, low, preferred_element_type=F32
    )


def entering(state, log_decay, rows, place, per_seq):
    total = state
    carried = jnp.zeros_like(state)
    bit = 1
    while bit < per_seq:
        other = swap(total, "seq", bit)
        upper = (place // bit) % 2 == 1
        reach = jnp.exp(log_decay * (rows * (place % bit)).astype(F32))[:, None, None]
        whole = jnp.exp(log_decay * float(rows * bit))[:, None, None]
        carried = carried + jnp.where(upper, reach * other, 0.0)
        if 2 * bit < per_seq:
            total = jnp.where(upper, whole * other + total, whole * total + other)
        bit *= 2
    return carried


def compute(
    layer_in,
    gain_one,
    w_query,
    w_key,
    w_value,
    w_gate,
    w_out,
    gain_two,
    w_ffgate,
    w_ffup,
    w_down,
    cotangent,
):
    rows, width = layer_in.shape
    half = rows // 2
    heads_here = w_query.shape[1] // DK
    heads_half = heads_here // 2
    n_seq = lax.axis_size("seq")
    n_head = lax.axis_size("head")
    seq_at = lax.axis_index("seq")
    head_at = lax.axis_index("head")
    side = seq_at % 2
    core = head_at % 2
    lines = [list(range(k, n_seq, 2)) for k in range(2)]
    own_row = core * half
    oth_row = half - own_row

    def row_part(value, start):
        return lax.dynamic_slice_in_dim(value, start, half, axis=0)

    def natural(own, other):
        return jnp.concatenate(
            [jnp.where(core == 0, own, other), jnp.where(core == 0, other, own)], axis=0
        )

    def head_sum(send_rows, keep_rows):
        total = keep_rows + swap(send_rows, "head", 1)
        bit = 2
        while bit < n_head:
            total = total + swap(total, "head", bit)
            bit *= 2
        return total

    def contract(a, b, dims):
        return lax.dot_general(a, b, (dims, ((), ())), preferred_element_type=F32)

    def dot(a, b):
        return contract(a, b, ((1,), (0,)))

    def dot_t(a, b):
        return contract(a, b, ((1,), (1,)))

    def tdot(a, b):
        return contract(a, b, ((0,), (0,)))

    def line_scatter(partial):
        return lax.psum_scatter(
            partial, "seq", scatter_dimension=0, tiled=True, axis_index_groups=lines
        )

    line = n_seq // 2
    folded = line == 4
    line_at = seq_at // 2
    line_half = line_at // (line // 2)
    inner = (line_at + line_half) % 2 == 1

    def along(value, hops):
        pairs = [(2 * a + k, 2 * b + k) for a, b in hops for k in range(2)]
        return lax.ppermute(value, "seq", pairs)

    def to_inner(value):
        return along(value, [(0, 1), (line - 1, line - 2)])

    def middle(value):
        return along(value, [(1, 2), (2, 1)])

    def to_end(value):
        return along(value, [(1, 0), (line - 2, line - 1)])

    def fold_grad(own, other, sides):
        own_z = to_inner(own)
        other_z = to_inner(other)
        every = (jnp.concatenate([own, other, own_z, other_z], axis=0) * 2.0).astype(BF16)
        far = tdot(sides[1], every)
        near = tdot(sides[0], every)
        total = near + middle(far)
        quarter = width // line
        end_rows = lax.dynamic_slice_in_dim(total, line_half * quarter, quarter, axis=0)
        inner_rows = lax.dynamic_slice_in_dim(total, quarter - line_half * quarter, quarter, axis=0)
        return jnp.where(inner, inner_rows, to_end(end_rows))

    def place_rows(reduced):
        mine = reduced.shape[0] // 2
        keep = lax.dynamic_slice_in_dim(reduced, side * mine, mine, axis=0)
        send = lax.dynamic_slice_in_dim(reduced, mine - side * mine, mine, axis=0)
        recv = swap(send, "seq", 1)
        return jnp.where(side == 0, keep, recv), jnp.where(side == 0, recv, keep)

    head_index = (head_at * heads_here + jnp.arange(heads_here)).astype(F32)
    log_decay = jnp.log(1.0 - jnp.exp2(-5.0 - head_index))
    decay_mask, lead_decay, tail_decay = decay_tables(log_decay, rows)
    per_seq = n_seq // SEQS
    place = seq_at % per_seq
    positions = place * rows + jnp.arange(rows)
    cos_part, sin_part = rotation(positions, DK // 2)
    scale = DK ** (-0.5)

    resid_in = layer_in.astype(F32)
    recip_one = lax.rsqrt(jnp.mean(resid_in * resid_in, axis=-1, keepdims=True) + EPS)
    scaled_one = resid_in * recip_one
    normed_one = (scaled_one * gain_one).astype(BF16)
    key_proj = dot(normed_one, w_key)
    value = dot(normed_one, w_value).astype(BF16)
    key_rot = (
        rotate(key_proj.reshape(rows, heads_here, DK), cos_part, sin_part)
        .astype(BF16)
        .transpose(1, 0, 2)
    )
    value_heads = value.reshape(rows, heads_here, DV).transpose(1, 0, 2)
    key_dec = (key_rot.astype(F32) * tail_decay).astype(BF16)
    local_state = jnp.einsum("hjd,hje->hde", key_dec, value_heads, preferred_element_type=F32)
    state_in = entering(local_state, log_decay, rows, place, per_seq)

    late_in, late_cot, late_one, late_recip, _ = lax.optimization_barrier(
        (layer_in, cotangent, normed_one, recip_one, local_state)
    )
    one_send = row_part(late_in, own_row).astype(F32) * row_part(late_recip, own_row)
    cot_send = row_part(late_cot, own_row).astype(F32) * 0.5
    one_own = swap(one_send, "seq", 1)
    one_oth = swap(one_own, "head", 1)
    normed_one_y = (natural(one_own, one_oth) * gain_one).astype(BF16)
    if folded:
        one_own_z = to_inner(one_send)
        one_own_zy = to_inner(one_own)
    cot_own_y = swap(cot_send, "seq", 1)
    cot_oth_y = swap(cot_own_y, "head", 1)

    query = dot(late_one, w_query)
    gate_pre = lax.optimization_barrier(dot(late_one, w_gate))
    query_rot = (
        (rotate(query.reshape(rows, heads_here, DK), cos_part, sin_part) * scale)
        .astype(BF16)
        .transpose(1, 0, 2)
    )
    scores = jnp.einsum("hid,hjd->hij", query_rot, key_rot, preferred_element_type=F32)
    weights_b = (scores * decay_mask).astype(BF16)
    retained = jnp.einsum("hij,hje->hie", weights_b, value_heads, preferred_element_type=F32)
    retained = lax.optimization_barrier(retained)
    retained = retained + split_dot(query_rot, state_in, "hid,hde->hie") * lead_decay
    normed_heads, inv_std = group_norm(retained)
    normed_tok = normed_heads.transpose(1, 0, 2).reshape(rows, heads_here * DV)
    gate_act = jax.nn.silu(gate_pre)
    gated = (gate_act * normed_tok).astype(BF16)

    mix_send = dot(row_part(gated, oth_row), w_out)
    mix_keep = dot(row_part(gated, own_row), w_out)
    resid_own = row_part(layer_in, own_row).astype(F32)
    hidden_own = resid_own + head_sum(mix_send, mix_keep)
    recip_two = lax.rsqrt(jnp.mean(hidden_own * hidden_own, axis=-1, keepdims=True) + EPS)
    two_own = hidden_own * recip_two
    two_oth = swap(two_own, "head", 1)
    normed_two = (jnp.concatenate([two_own, two_oth], axis=0) * gain_two).astype(BF16)

    cot_own = row_part(cotangent, own_row)
    cot_oth = row_part(cotangent, oth_row)
    cot_perm = jnp.concatenate([cot_own, cot_oth], axis=0)
    d_inner = dot_t(cot_perm, w_down)
    ff_gate = dot(normed_two, w_ffgate)
    ff_up = dot(normed_two, w_ffup)
    ff_act, gelu_back = jax.vjp(gelu_tanh, ff_gate)
    inner_act = (ff_act * ff_up).astype(BF16)
    d_ffgate_f = gelu_back(d_inner * ff_up)[0]
    d_ffup_f = d_inner * ff_act
    d_ffgate = d_ffgate_f.astype(BF16)
    d_ffup = d_ffup_f.astype(BF16)

    def two_part(gate_rows, up_rows):
        return dot_t(gate_rows, w_ffgate) + dot_t(up_rows, w_ffup)

    two_send = two_part(d_ffgate[half:], d_ffup[half:])
    two_keep = two_part(d_ffgate[:half], d_ffup[:half])
    d_normtwo = head_sum(two_send, two_keep)

    across = (head_at // 2) % 2
    if n_head % 4 == 0:
        span = width // 2
        two_piece = lax.dynamic_slice_in_dim(two_own, across * span, span, axis=1)
        two_piece_y = swap(two_piece, "seq", 1)
        two_piece_x = swap(two_piece_y, "head", 2)
        two_own_y = jnp.concatenate(
            [
                jnp.where(across == 0, two_piece_y, two_piece_x),
                jnp.where(across == 0, two_piece_x, two_piece_y),
            ],
            axis=1,
        )
    else:
        two_own_y = swap(two_own, "seq", 1)
    two_oth_y = swap(two_own_y, "head", 1)
    normed_two_y = (jnp.concatenate([two_own_y, two_oth_y], axis=0) * gain_two).astype(BF16)
    cot_perm_y = (jnp.concatenate([cot_own_y, cot_oth_y], axis=0) * 2.0).astype(BF16)

    ff_half = inner_act.shape[1] // 2
    inner_f = ff_act * ff_up
    inner_send = jnp.where(side == 0, inner_f[:, ff_half:], inner_f[:, :ff_half]) * 0.5
    inner_keep = jnp.where(side == 0, inner_act[:, :ff_half], inner_act[:, ff_half:])
    inner_recv = (swap(inner_send, "seq", 1) * 2.0).astype(BF16)
    red_down = line_scatter(tdot(cot_perm, inner_keep) + tdot(cot_perm_y, inner_recv))

    dff_send = jnp.where(side == 0, d_ffup_f, d_ffgate_f) * 0.5
    dff_keep = jnp.where(side == 0, d_ffgate, d_ffup)
    dff_recv = (swap(dff_send, "seq", 1) * 2.0).astype(BF16)
    red_ff = line_scatter(tdot(normed_two, dff_keep) + tdot(normed_two_y, dff_recv))

    d_hidden_norm, gain_two_part = rms_backward(hidden_own, recip_two, gain_two, d_normtwo)
    dhn_oth = swap(d_hidden_norm, "head", 1)
    d_hidden_own = cot_own.astype(F32) + d_hidden_norm
    d_hidden_b = natural(d_hidden_own, cot_oth.astype(F32) + dhn_oth).astype(BF16)

    ffn_send = dot(inner_act[half:], w_down)
    ffn_keep = dot(inner_act[:half], w_down)
    ffn_sum = head_sum(ffn_send, ffn_keep)

    d_gated = dot_t(d_hidden_b, w_out)
    d_gatepre_f = d_gated * normed_tok * silu_slope(gate_pre)
    d_normed = (d_gated * gate_act).reshape(rows, heads_here, DV).transpose(1, 0, 2)
    d_ret_b = group_norm_back(normed_heads, inv_std, d_normed).astype(BF16)
    late_hidden, d_ret_b, late_pre = lax.optimization_barrier((hidden_own, d_ret_b, d_gatepre_f))
    d_gatepre = late_pre.astype(BF16)
    out_own = late_hidden + ffn_sum
    out_oth = swap(out_own * 0.5, "head", 1) * 2.0
    layer_out = natural(out_own, out_oth).astype(BF16)
    query_dec = (query_rot.astype(F32) * lead_decay).astype(BF16)
    d_state = jnp.einsum("hid,hie->hde", query_dec, d_ret_b, preferred_element_type=F32)
    carried_back = entering(d_state, log_decay, rows, per_seq - 1 - place, per_seq)

    dhn_send = d_hidden_norm
    dhn_own_y = swap(dhn_send, "seq", 1)
    dhn_oth_y = swap(dhn_own_y, "head", 1)
    d_hidden_b_y = natural(
        cot_own_y * 2.0 + dhn_own_y, cot_oth_y * 2.0 + dhn_oth_y
    ).astype(BF16)

    wide = heads_half * DV

    def cols(value, which):
        return lax.dynamic_slice_in_dim(value, which * wide, wide, axis=1)

    gated_f = gate_act * normed_tok
    gated_recv = (swap(cols(gated_f, 1 - side) * 0.5, "seq", 1) * 2.0).astype(BF16)
    gate_recv = swap(cols(late_pre, 1 - side) * 0.5, "seq", 1)
    if folded:
        one_z = jnp.concatenate([one_own_z, one_own_zy], axis=0)
        one_zc = swap(one_z, "head", 1)
        one_all = jnp.concatenate(
            [
                normed_one,
                normed_one_y,
                (natural(one_own_z, one_zc[:half]) * gain_one).astype(BF16),
                (natural(one_own_zy, one_zc[half:]) * gain_one).astype(BF16),
            ],
            axis=0,
        )
        spread = width // 2
        ones = tuple(
            lax.dynamic_slice_in_dim(one_all, part * spread, spread, axis=1)
            for part in (line_half, 1 - line_half)
        )
        red_gate = fold_grad(cols(late_pre, side) * 0.5, gate_recv, ones)
    else:
        red_gate = line_scatter(
            tdot(normed_one, cols(d_gatepre, side))
            + tdot(normed_one_y, (gate_recv * 2.0).astype(BF16)),
        )
    red_out = line_scatter(tdot(d_hidden_b, cols(gated, side)) + tdot(d_hidden_b_y, gated_recv))

    d_raw = jnp.einsum("hie,hje->hij", d_ret_b, value_heads, preferred_element_type=F32)
    d_weights = (d_raw * decay_mask).astype(BF16)
    d_query = jnp.einsum("hij,hjd->hid", d_weights, key_rot, preferred_element_type=F32)
    d_query = d_query + split_dot(d_ret_b, state_in, "hie,hde->hid") * lead_decay
    d_key = jnp.einsum("hij,hid->hjd", d_weights, query_rot, preferred_element_type=F32)
    d_key = d_key + split_dot(value_heads, carried_back, "hje,hde->hjd") * tail_decay
    d_value = jnp.einsum("hij,hie->hje", weights_b, d_ret_b, preferred_element_type=F32)
    d_value = d_value + split_dot(key_rot, carried_back, "hjd,hde->hje") * tail_decay
    d_query = unrotate(d_query, cos_part, sin_part) * scale
    d_key = unrotate(d_key, cos_part, sin_part)
    d_query_b, d_key_b, d_value_b = (v.astype(BF16) for v in (d_query, d_key, d_value))

    def tokens(value):
        return value.transpose(1, 0, 2).reshape(rows, -1)

    def head_half(value, which):
        part = lax.dynamic_slice_in_dim(value, which * heads_half, heads_half, axis=0)
        return tokens(part)

    def both(values, which):
        return jnp.concatenate([head_half(v, which) for v in values], axis=1)

    value_recv = swap(head_half(d_value, 1 - side) * 0.5, "seq", 1)
    qk_recv = swap(both((d_query, d_key), 1 - side) * 0.5, "seq", 1)
    red_v = line_scatter(
        tdot(normed_one, head_half(d_value_b, side))
        + tdot(normed_one_y, (value_recv * 2.0).astype(BF16)),
    )
    red_qk = line_scatter(
        tdot(normed_one, both((d_query_b, d_key_b), side))
        + tdot(normed_one_y, (qk_recv * 2.0).astype(BF16)),
    )

    dq_tok, dk_tok, dv_tok = tokens(d_query_b), tokens(d_key_b), tokens(d_value_b)

    def one_part(start):
        return (
            dot_t(row_part(dq_tok, start), w_query)
            + dot_t(row_part(dk_tok, start), w_key)
            + dot_t(row_part(d_gatepre, start), w_gate)
            + dot_t(row_part(dv_tok, start), w_value)
        )

    d_normone = head_sum(one_part(oth_row), one_part(own_row))
    d_input_norm, gain_one_part = rms_backward(
        resid_own, row_part(recip_one, own_row), gain_one, d_normone
    )
    grad_own = d_hidden_own + d_input_norm
    grad_input = natural(grad_own, swap(grad_own, "head", 1))

    gains = jnp.stack([gain_one_part, gain_two_part])
    gains = gains + swap(gains, "head", 1)
    bit = 1
    while bit < n_seq:
        gains = gains + swap(gains, "seq", bit)
        bit *= 2
    chunk = width // n_seq
    gains = lax.dynamic_slice_in_dim(gains, seq_at * chunk, chunk, axis=1)

    down_lo, down_hi = place_rows(red_down)
    grad_down = jnp.concatenate([down_lo, down_hi], axis=1).T
    grad_ffgate, grad_ffup = place_rows(red_ff)
    grad_gate = jnp.concatenate(place_rows(red_gate), axis=1)
    grad_out = jnp.concatenate(place_rows(red_out), axis=1).T
    grad_value = jnp.concatenate(place_rows(red_v), axis=1)
    qk_lo, qk_hi = place_rows(red_qk)
    kw = heads_half * DK
    grad_query = jnp.concatenate([qk_lo[:, :kw], qk_hi[:, :kw]], axis=1)
    grad_key = jnp.concatenate([qk_lo[:, kw:], qk_hi[:, kw:]], axis=1)
    return (
        layer_out,
        grad_input,
        gains[0],
        grad_query,
        grad_key,
        grad_value,
        grad_gate,
        grad_out,
        gains[1],
        grad_ffgate,
        grad_ffup,
        grad_down,
    )


def solution(mesh):
    in_specs = (
        P("seq", None),
        P(),
        P(None, "head"),
        P(None, "head"),
        P(None, "head"),
        P(None, "head"),
        P("head", None),
        P(),
        P(None, "head"),
        P(None, "head"),
        P("head", None),
        P("seq", None),
    )
    out_specs = (
        P("seq", None),
        P("seq", None),
        P("seq"),
        P("seq", "head"),
        P("seq", "head"),
        P("seq", "head"),
        P("seq", "head"),
        P("head", "seq"),
        P("seq"),
        P("seq", "head"),
        P("seq", "head"),
        P("head", "seq"),
    )
    return jax.shard_map(compute, mesh=mesh, in_specs=in_specs, out_specs=out_specs, check_vma=False)
```

```python
import jax
import jax.numpy as jnp
from jax import lax
from jax.sharding import PartitionSpec as P


DK = 256
DV = 512
SEQS = 2

EPS = 1e-05
ROPE_BASE = 10000.0
F32 = jnp.float32
BF16 = jnp.bfloat16


def swap(value, axis, bit):
    count = lax.axis_size(axis)
    return lax.ppermute(value, axis, [(i, i ^ bit) for i in range(count)])


def rotation(positions, half_dim):
    frequency = ROPE_BASE ** (-jnp.arange(half_dim, dtype=F32) / half_dim)
    angles = positions.astype(F32)[:, None] * frequency[None, :]
    return (jnp.cos(angles), jnp.sin(angles))


def rotate(values, cos_part, sin_part):
    half_dim = cos_part.shape[1]
    leading = values[..., :half_dim]
    trailing = values[..., half_dim:]
    cos_wide = cos_part[:, None, :]
    sin_wide = sin_part[:, None, :]
    return jnp.concatenate(
        [leading * cos_wide - trailing * sin_wide, trailing * cos_wide + leading * sin_wide],
        axis=-1,
    )


def unrotate(gradient, cos_part, sin_part):
    half_dim = cos_part.shape[1]
    leading = gradient[..., :half_dim]
    trailing = gradient[..., half_dim:]
    return jnp.concatenate(
        [leading * cos_part + trailing * sin_part, trailing * cos_part - leading * sin_part],
        axis=-1,
    )


def group_norm(retained):
    centred = retained - jnp.mean(retained, axis=-1, keepdims=True)
    inv_std = lax.rsqrt(jnp.mean(centred * centred, axis=-1, keepdims=True) + EPS)
    return (centred * inv_std, inv_std)


def group_norm_back(normed, inv_std, upstream):
    first_mean = jnp.mean(upstream, axis=-1, keepdims=True)
    second_mean = jnp.mean(upstream * normed, axis=-1, keepdims=True)
    return inv_std * (upstream - first_mean - normed * second_mean)


def silu_slope(inputs):
    sigmoid = jax.nn.sigmoid(inputs)
    return sigmoid * (1.0 + inputs * (1.0 - sigmoid))


def rms_backward(inputs, recip, gain_vec, upstream):
    weighted = upstream * gain_vec
    inner_mean = jnp.mean(weighted * inputs, axis=-1, keepdims=True)
    grad_in = recip * weighted - inputs * (recip * recip * recip) * inner_mean
    grad_gain = jnp.sum(upstream * inputs * recip, axis=0)
    return (grad_in, grad_gain)


def decay_tables(log_decay, rows):
    steps_in = jnp.arange(rows, dtype=F32)
    offset = steps_in[:, None] - steps_in[None, :]
    decay_mask = jnp.where(
        offset[None] >= 0.0, jnp.exp(log_decay[:, None, None] * jnp.maximum(offset, 0.0)[None]), 0.0
    )
    lead_decay = jnp.exp(log_decay[:, None] * (steps_in + 1.0))[:, :, None]
    tail_decay = jnp.exp(log_decay[:, None] * (rows - 1.0 - steps_in))[:, :, None]
    return (decay_mask, lead_decay, tail_decay)


def gelu_tanh(inputs):
    return jax.nn.gelu(inputs, approximate=True)


def split_dot(lhs, rhs, spec):
    high = rhs.astype(BF16)
    low = (rhs - high.astype(F32)).astype(BF16)
    return jnp.einsum(spec, lhs, high, preferred_element_type=F32) + jnp.einsum(
        spec, lhs, low, preferred_element_type=F32
    )


def entering(state, log_decay, rows, place, per_seq):
    total = state
    carried = jnp.zeros_like(state)
    bit = 1
    while bit < per_seq:
        other = swap(total, "seq", bit)
        upper = (place // bit) % 2 == 1
        reach = jnp.exp(log_decay * (rows * (place % bit)).astype(F32))[:, None, None]
        whole = jnp.exp(log_decay * float(rows * bit))[:, None, None]
        carried = carried + jnp.where(upper, reach * other, 0.0)
        if 2 * bit < per_seq:
            total = jnp.where(upper, whole * other + total, whole * total + other)
        bit *= 2
    return carried


def compute(
    layer_in,
    gain_one,
    w_query,
    w_key,
    w_value,
    w_gate,
    w_out,
    gain_two,
    w_ffgate,
    w_ffup,
    w_down,
    cotangent,
):
    rows, width = layer_in.shape
    half = rows // 2
    heads_here = w_query.shape[1] // DK
    heads_half = heads_here // 2
    n_seq = lax.axis_size("seq")
    n_head = lax.axis_size("head")
    seq_at = lax.axis_index("seq")
    head_at = lax.axis_index("head")
    side = seq_at % 2
    core = head_at % 2
    lines = [list(range(k, n_seq, 2)) for k in range(2)]
    own_row = core * half
    oth_row = half - own_row

    def row_part(value, start):
        return lax.dynamic_slice_in_dim(value, start, half, axis=0)

    def natural(own, other):
        return jnp.concatenate(
            [jnp.where(core == 0, own, other), jnp.where(core == 0, other, own)], axis=0
        )

    def head_sum(send_rows, keep_rows):
        total = keep_rows + swap(send_rows, "head", 1)
        bit = 2
        while bit < n_head:
            total = total + swap(total, "head", bit)
            bit *= 2
        return total

    def contract(a, b, dims):
        return lax.dot_general(a, b, (dims, ((), ())), preferred_element_type=F32)

    def dot(a, b):
        return contract(a, b, ((1,), (0,)))

    def dot_t(a, b):
        return contract(a, b, ((1,), (1,)))

    def tdot(a, b):
        return contract(a, b, ((0,), (0,)))

    def line_scatter(partial):
        return lax.psum_scatter(
            partial, "seq", scatter_dimension=0, tiled=True, axis_index_groups=lines
        )

    def place_rows(reduced):
        mine = reduced.shape[0] // 2
        keep = lax.dynamic_slice_in_dim(reduced, side * mine, mine, axis=0)
        send = lax.dynamic_slice_in_dim(reduced, mine - side * mine, mine, axis=0)
        recv = swap(send, "seq", 1)
        return jnp.where(side == 0, keep, recv), jnp.where(side == 0, recv, keep)

    head_index = (head_at * heads_here + jnp.arange(heads_here)).astype(F32)
    log_decay = jnp.log(1.0 - jnp.exp2(-5.0 - head_index))
    decay_mask, lead_decay, tail_decay = decay_tables(log_decay, rows)
    per_seq = n_seq // SEQS
    place = seq_at % per_seq
    positions = place * rows + jnp.arange(rows)
    cos_part, sin_part = rotation(positions, DK // 2)
    scale = DK ** (-0.5)

    resid_in = layer_in.astype(F32)
    recip_one = lax.rsqrt(jnp.mean(resid_in * resid_in, axis=-1, keepdims=True) + EPS)
    scaled_one = resid_in * recip_one
    normed_one = (scaled_one * gain_one).astype(BF16)
    key_proj = dot(normed_one, w_key)
    value = dot(normed_one, w_value).astype(BF16)
    key_rot = (
        rotate(key_proj.reshape(rows, heads_here, DK), cos_part, sin_part)
        .astype(BF16)
        .transpose(1, 0, 2)
    )
    value_heads = value.reshape(rows, heads_here, DV).transpose(1, 0, 2)
    key_dec = (key_rot.astype(F32) * tail_decay).astype(BF16)
    local_state = jnp.einsum("hjd,hje->hde", key_dec, value_heads, preferred_element_type=F32)
    state_in = entering(local_state, log_decay, rows, place, per_seq)

    late_in, late_cot, late_one, late_recip, _ = lax.optimization_barrier(
        (layer_in, cotangent, normed_one, recip_one, local_state)
    )
    one_send = row_part(late_in, own_row).astype(F32) * row_part(late_recip, own_row)
    cot_send = row_part(late_cot, own_row).astype(F32) * 0.5
    one_own = swap(one_send, "seq", 1)
    one_oth = swap(one_own, "head", 1)
    normed_one_y = (natural(one_own, one_oth) * gain_one).astype(BF16)
    cot_own_y = swap(cot_send, "seq", 1)
    cot_oth_y = swap(cot_own_y, "head", 1)

    query = dot(late_one, w_query)
    gate_pre = lax.optimization_barrier(dot(late_one, w_gate))
    query_rot = (
        (rotate(query.reshape(rows, heads_here, DK), cos_part, sin_part) * scale)
        .astype(BF16)
        .transpose(1, 0, 2)
    )
    scores = jnp.einsum("hid,hjd->hij", query_rot, key_rot, preferred_element_type=F32)
    weights_b = (scores * decay_mask).astype(BF16)
    retained = jnp.einsum("hij,hje->hie", weights_b, value_heads, preferred_element_type=F32)
    retained = lax.optimization_barrier(retained)
    retained = retained + split_dot(query_rot, state_in, "hid,hde->hie") * lead_decay
    normed_heads, inv_std = group_norm(retained)
    normed_tok = normed_heads.transpose(1, 0, 2).reshape(rows, heads_here * DV)
    gate_act = jax.nn.silu(gate_pre)
    gated = (gate_act * normed_tok).astype(BF16)

    mix_send = dot(row_part(gated, oth_row), w_out)
    mix_keep = dot(row_part(gated, own_row), w_out)
    resid_own = row_part(layer_in, own_row).astype(F32)
    hidden_own = resid_own + head_sum(mix_send, mix_keep)
    recip_two = lax.rsqrt(jnp.mean(hidden_own * hidden_own, axis=-1, keepdims=True) + EPS)
    two_own = hidden_own * recip_two
    two_oth = swap(two_own, "head", 1)
    normed_two = (jnp.concatenate([two_own, two_oth], axis=0) * gain_two).astype(BF16)

    cot_own = row_part(cotangent, own_row)
    cot_oth = row_part(cotangent, oth_row)
    cot_perm = jnp.concatenate([cot_own, cot_oth], axis=0)
    d_inner = dot_t(cot_perm, w_down)
    ff_gate = dot(normed_two, w_ffgate)
    ff_up = dot(normed_two, w_ffup)
    ff_act, gelu_back = jax.vjp(gelu_tanh, ff_gate)
    inner_act = (ff_act * ff_up).astype(BF16)
    d_ffgate_f = gelu_back(d_inner * ff_up)[0]
    d_ffup_f = d_inner * ff_act
    d_ffgate = d_ffgate_f.astype(BF16)
    d_ffup = d_ffup_f.astype(BF16)

    def two_part(gate_rows, up_rows):
        return dot_t(gate_rows, w_ffgate) + dot_t(up_rows, w_ffup)

    two_send = two_part(d_ffgate[half:], d_ffup[half:])
    two_keep = two_part(d_ffgate[:half], d_ffup[:half])
    d_normtwo = head_sum(two_send, two_keep)

    across = (head_at // 2) % 2
    if n_head % 4 == 0:
        span = width // 2
        two_piece = lax.dynamic_slice_in_dim(two_own, across * span, span, axis=1)
        two_piece_y = swap(two_piece, "seq", 1)
        two_piece_x = swap(two_piece_y, "head", 2)
        two_own_y = jnp.concatenate(
            [
                jnp.where(across == 0, two_piece_y, two_piece_x),
                jnp.where(across == 0, two_piece_x, two_piece_y),
            ],
            axis=1,
        )
    else:
        two_own_y = swap(two_own, "seq", 1)
    two_oth_y = swap(two_own_y, "head", 1)
    normed_two_y = (jnp.concatenate([two_own_y, two_oth_y], axis=0) * gain_two).astype(BF16)
    cot_perm_y = (jnp.concatenate([cot_own_y, cot_oth_y], axis=0) * 2.0).astype(BF16)

    ff_half = inner_act.shape[1] // 2
    inner_f = ff_act * ff_up
    inner_send = jnp.where(side == 0, inner_f[:, ff_half:], inner_f[:, :ff_half]) * 0.5
    inner_keep = jnp.where(side == 0, inner_act[:, :ff_half], inner_act[:, ff_half:])
    inner_recv = (swap(inner_send, "seq", 1) * 2.0).astype(BF16)
    red_down = line_scatter(tdot(cot_perm, inner_keep) + tdot(cot_perm_y, inner_recv))

    dff_send = jnp.where(side == 0, d_ffup_f, d_ffgate_f) * 0.5
    dff_keep = jnp.where(side == 0, d_ffgate, d_ffup)
    dff_recv = (swap(dff_send, "seq", 1) * 2.0).astype(BF16)
    red_ff = line_scatter(tdot(normed_two, dff_keep) + tdot(normed_two_y, dff_recv))

    d_hidden_norm, gain_two_part = rms_backward(hidden_own, recip_two, gain_two, d_normtwo)
    dhn_oth = swap(d_hidden_norm, "head", 1)
    d_hidden_own = cot_own.astype(F32) + d_hidden_norm
    d_hidden_b = natural(d_hidden_own, cot_oth.astype(F32) + dhn_oth).astype(BF16)

    ffn_send = dot(inner_act[half:], w_down)
    ffn_keep = dot(inner_act[:half], w_down)
    ffn_sum = head_sum(ffn_send, ffn_keep)

    d_gated = dot_t(d_hidden_b, w_out)
    d_gatepre_f = d_gated * normed_tok * silu_slope(gate_pre)
    d_normed = (d_gated * gate_act).reshape(rows, heads_here, DV).transpose(1, 0, 2)
    d_ret_b = group_norm_back(normed_heads, inv_std, d_normed).astype(BF16)
    late_hidden, d_ret_b, late_pre = lax.optimization_barrier((hidden_own, d_ret_b, d_gatepre_f))
    d_gatepre = late_pre.astype(BF16)
    out_own = late_hidden + ffn_sum
    out_oth = swap(out_own * 0.5, "head", 1) * 2.0
    layer_out = natural(out_own, out_oth).astype(BF16)
    query_dec = (query_rot.astype(F32) * lead_decay).astype(BF16)
    d_state = jnp.einsum("hid,hie->hde", query_dec, d_ret_b, preferred_element_type=F32)
    carried_back = entering(d_state, log_decay, rows, per_seq - 1 - place, per_seq)

    dhn_send = d_hidden_norm
    dhn_own_y = swap(dhn_send, "seq", 1)
    dhn_oth_y = swap(dhn_own_y, "head", 1)
    d_hidden_b_y = natural(
        cot_own_y * 2.0 + dhn_own_y, cot_oth_y * 2.0 + dhn_oth_y
    ).astype(BF16)

    wide = heads_half * DV

    def cols(value, which):
        return lax.dynamic_slice_in_dim(value, which * wide, wide, axis=1)

    gated_f = gate_act * normed_tok
    gated_recv = (swap(cols(gated_f, 1 - side) * 0.5, "seq", 1) * 2.0).astype(BF16)
    gate_recv = (swap(cols(late_pre, 1 - side) * 0.5, "seq", 1) * 2.0).astype(BF16)
    red_gate = line_scatter(tdot(normed_one, cols(d_gatepre, side)) + tdot(normed_one_y, gate_recv))
    d_raw = jnp.einsum("hie,hje->hij", d_ret_b, value_heads, preferred_element_type=F32)
    d_weights = (d_raw * decay_mask).astype(BF16)
    d_query = jnp.einsum("hij,hjd->hid", d_weights, key_rot, preferred_element_type=F32)
    d_query = d_query + split_dot(d_ret_b, state_in, "hie,hde->hid") * lead_decay
    d_key = jnp.einsum("hij,hid->hjd", d_weights, query_rot, preferred_element_type=F32)
    d_key = d_key + split_dot(value_heads, carried_back, "hje,hde->hjd") * tail_decay
    d_value = jnp.einsum("hij,hie->hje", weights_b, d_ret_b, preferred_element_type=F32)
    d_value = d_value + split_dot(key_rot, carried_back, "hjd,hde->hje") * tail_decay
    d_query = unrotate(d_query, cos_part, sin_part) * scale
    d_key = unrotate(d_key, cos_part, sin_part)
    d_query_b, d_key_b, d_value_b = (v.astype(BF16) for v in (d_query, d_key, d_value))

    def tokens(value):
        return value.transpose(1, 0, 2).reshape(rows, -1)

    def head_half(value, which):
        part = lax.dynamic_slice_in_dim(value, which * heads_half, heads_half, axis=0)
        return tokens(part)

    qkv_send = jnp.concatenate([head_half(v, 1 - side) for v in (d_value, d_query, d_key)], axis=1)
    qkv_recv = (swap(qkv_send * 0.5, "seq", 1) * 2.0).astype(BF16)
    qk_keep = jnp.concatenate([head_half(v, side) for v in (d_query_b, d_key_b)], axis=1)
    out_part = tdot(d_hidden_b, cols(gated, side)) + tdot(d_hidden_b_y, gated_recv)
    v_part = tdot(normed_one, head_half(d_value_b, side)) + tdot(normed_one_y, qkv_recv[:, :wide])
    red_ov = line_scatter(jnp.concatenate([out_part, v_part], axis=1))
    red_qk = line_scatter(tdot(normed_one, qk_keep) + tdot(normed_one_y, qkv_recv[:, wide:]))

    dq_tok, dk_tok, dv_tok = tokens(d_query_b), tokens(d_key_b), tokens(d_value_b)

    def one_part(start):
        return (
            dot_t(row_part(dq_tok, start), w_query)
            + dot_t(row_part(dk_tok, start), w_key)
            + dot_t(row_part(d_gatepre, start), w_gate)
            + dot_t(row_part(dv_tok, start), w_value)
        )

    d_normone = head_sum(one_part(oth_row), one_part(own_row))
    d_input_norm, gain_one_part = rms_backward(
        resid_own, row_part(recip_one, own_row), gain_one, d_normone
    )
    grad_own = d_hidden_own + d_input_norm
    grad_input = natural(grad_own, swap(grad_own, "head", 1))

    gains = jnp.stack([gain_one_part, gain_two_part])
    gains = gains + swap(gains, "head", 1)
    bit = 1
    while bit < n_seq:
        gains = gains + swap(gains, "seq", bit)
        bit *= 2
    chunk = width // n_seq
    gains = lax.dynamic_slice_in_dim(gains, seq_at * chunk, chunk, axis=1)

    down_lo, down_hi = place_rows(red_down)
    grad_down = jnp.concatenate([down_lo, down_hi], axis=1).T
    grad_ffgate, grad_ffup = place_rows(red_ff)
    grad_gate = jnp.concatenate(place_rows(red_gate), axis=1)
    ov_lo, ov_hi = place_rows(red_ov)
    grad_out = jnp.concatenate([ov_lo[:, :wide], ov_hi[:, :wide]], axis=1).T
    grad_value = jnp.concatenate([ov_lo[:, wide:], ov_hi[:, wide:]], axis=1)
    qk_lo, qk_hi = place_rows(red_qk)
    kw = heads_half * DK
    grad_query = jnp.concatenate([qk_lo[:, :kw], qk_hi[:, :kw]], axis=1)
    grad_key = jnp.concatenate([qk_lo[:, kw:], qk_hi[:, kw:]], axis=1)
    return (
        layer_out,
        grad_input,
        gains[0],
        grad_query,
        grad_key,
        grad_value,
        grad_gate,
        grad_out,
        gains[1],
        grad_ffgate,
        grad_ffup,
        grad_down,
    )


def solution(mesh):
    in_specs = (
        P("seq", None),
        P(),
        P(None, "head"),
        P(None, "head"),
        P(None, "head"),
        P(None, "head"),
        P("head", None),
        P(),
        P(None, "head"),
        P(None, "head"),
        P("head", None),
        P("seq", None),
    )
    out_specs = (
        P("seq", None),
        P("seq", None),
        P("seq"),
        P("seq", "head"),
        P("seq", "head"),
        P("seq", "head"),
        P("seq", "head"),
        P("head", "seq"),
        P("seq"),
        P("seq", "head"),
        P("seq", "head"),
        P("head", "seq"),
    )
    return jax.shard_map(compute, mesh=mesh, in_specs=in_specs, out_specs=out_specs, check_vma=False)
```
